32 devices in a mesh: grp: 4 (over y, x), own: 8 (over z, core).
Axes of the slice: x: 2, y: 2, z: 4, core: 2. Of those that a mesh axis runs over, the one named last changes fastest.
Arguments:
- tile_row: int32 [4, 8, 1536], P('grp', 'own'), may hold values from 0 to 7
- pixel_col: int32 [4, 8, 1536], P('grp', 'own'), may hold values from 0 to 16383
- weight: bfloat16 [4, 8, 1536], P('grp', 'own'), may hold values from 0.25 to 4
- counts: int32 [4, 8, 8], P('grp', 'own'), may hold values from 1 to 192
- kernel: float32 [9, 9], replicated, may hold values from 0.01 to 0.05
Outputs:
- smoothed: float32 [64, 16384], P('own', 'grp')
The draws below stay inside these ranges and needn't reach their ends.
Inputs may be any that keep to these rules, and one draw needn't show every extreme that they name: `counts`: slots past a block's count hold unused values.
All inputs are finite; a program needn't handle non-finite values.
Results may differ from the reference program's by a relative error of at most 0.0012.
Values may be sent and summed in bfloat16 or wider, within the bound.
A program may use at most 64 MiB of HBM per device.

```python
import math
import jax
import jax.numpy as jnp

W = 16384
STRIP = 8
CAP = 192
NROWS = 64
N_GRP = 4
N_OWN = 8


def with_ends(array, rng, low, top_value):
    place = [jax.random.randint(jax.random.fold_in(rng, axis), (), 0, length) for axis, length in enumerate(array.shape)]
    longest = array.shape.index(max(array.shape))
    neighbour = place[:longest] + [(place[longest] + 1) % array.shape[longest]] + place[longest + 1:]
    return array.at[tuple(place)].set(low).at[tuple(neighbour)].set(top_value)


def level_of(own_key, shape, shards, least, high):
    level = 1.0
    for dim, parts in shards:
        steps = jax.random.uniform(jax.random.fold_in(jax.random.fold_in(own_key, 6), dim), (parts,), jnp.float32, least / len(shards), high / len(shards))
        level = level * jnp.repeat(jnp.exp(steps), shape[dim] // parts).reshape((-1,) + (1,) * (len(shape) - 1 - dim))
    return level


def setup_inputs(seed: int = 0) -> dict:
    seeds = jax.random.split(jax.random.key(seed), 6)
    return {
        "tile_row": with_ends(jax.random.randint(seeds[0], (N_GRP, N_OWN, N_OWN * CAP), 0, STRIP), jax.random.fold_in(seeds[0], 1), 0, STRIP - 1).astype(jnp.int32),
        "pixel_col": with_ends(jax.random.randint(seeds[1], (N_GRP, N_OWN, N_OWN * CAP), 0, W), jax.random.fold_in(seeds[1], 1), 0, W - 1).astype(jnp.int32),
        "weight": jnp.clip(jnp.exp(math.log(4.0) - 2.7725887 * jax.random.uniform(seeds[2], (N_GRP, N_OWN, N_OWN * CAP), jnp.float32) ** level_of(seeds[2], (N_GRP, N_OWN, N_OWN * CAP), ((0, 4), (1, 8)), -0.2, 0.2)), 0.25, 4.0).astype(jnp.bfloat16),
        "counts": with_ends(jax.random.randint(seeds[3], (N_GRP, N_OWN, N_OWN), 1, CAP + 1), jax.random.fold_in(seeds[3], 1), 1, CAP).astype(jnp.int32),
        "kernel": jnp.clip(jax.random.uniform(seeds[4], (9, 9), jnp.float32, 0.01, 0.05), 0.01, 0.05),
    }


def reference(tile_row, pixel_col, weight, counts, kernel):
    slot_count = tile_row.shape[2]
    slot_ids = jnp.arange(slot_count, dtype=jnp.int32)
    dest_ids = slot_ids // CAP
    live = (slot_ids % CAP)[None, None, :] < jnp.repeat(counts, CAP, axis=2)
    grid_row = dest_ids[None, None, :] * STRIP + tile_row
    flat_index = (grid_row * W + pixel_col).astype(jnp.int32).reshape(-1)
    values = jnp.where(live, weight.astype(jnp.float32), jnp.zeros((), jnp.float32)).reshape(-1)
    heat = jax.ops.segment_sum(values, flat_index, num_segments=NROWS * W).reshape(NROWS, W)
    padded = jnp.pad(heat, 4)
    smoothed = jnp.zeros((NROWS, W), jnp.float32)
    for a in range(9):
        for b in range(9):
            smoothed = smoothed + kernel[a, b] * padded[a:a + NROWS, b:b + W]
    return smoothed
```

```python
import functools
import math

import jax
import jax.numpy as jnp
from jax import lax
from jax.experimental import pallas as pl
from jax.experimental.pallas import tpu as pltpu
from jax.sharding import PartitionSpec as P

W = 16384
STRIP = 8
REACH = 4
TAPS = 9
LANES = 256
CHUNK = 512
BATCH = 4
MESH = pl.DeviceIdType.MESH


def heat_kernel(
    n_g, n_o, cap, span, row_ref, col_ref, weight_ref, counts_ref, kern_ref, out_ref,
    stage, recv, acc, halo_out, halo_in, ext,
    send_sem, recv_sem, halo_send_sem, halo_recv_sem,
):
    n = n_g * n_o
    me_g, me_o = lax.axis_index("grp"), lax.axis_index("own")
    me = me_g * n_o + me_o
    quarter = out_ref.shape[1]
    slots = row_ref.shape[2]
    tiles = acc.shape[0] // STRIP

    barrier = pltpu.get_barrier_semaphore()

    def greet(k, carry):
        peer = lax.rem(me + k, n)
        pl.semaphore_signal(
            barrier, inc=1, device_id=(lax.div(peer, n_o), lax.rem(peer, n_o)), device_id_type=MESH
        )
        return carry

    lax.fori_loop(1, n, greet, 0)

    period = math.lcm(cap, 128)
    per = period // cap

    def prepare(k, carry):
        at = pl.ds(pl.multiple_of(k * period, 128), period)
        lane = lax.broadcasted_iota(jnp.int32, (1, period), 1)
        limit = jnp.full((1, period), counts_ref[0, 0, k * per], jnp.int32)
        for j in range(1, per):
            limit = jnp.where(lane >= j * cap, counts_ref[0, 0, k * per + j] + j * cap, limit)
        index = row_ref[0, :, at] * W + col_ref[0, :, at]
        stage[0:1, at] = index.astype(jnp.float32)
        stage[1:2, at] = jnp.where(lane < limit, weight_ref[0, :, at].astype(jnp.float32), 0.0)
        return carry

    lax.fori_loop(0, slots // period, prepare, 0)
    for k in range(halo_in.shape[0]):
        halo_in_zero = jnp.zeros(halo_in.shape[1:], halo_in.dtype)

        @pl.when(me_o == (0 if k == 0 else n_o - 1))
        def _():
            halo_in[k] = halo_in_zero

    acc[...] = jnp.zeros_like(acc)

    def window(owner):
        return pl.ds(pl.multiple_of(lax.div(owner * cap, 128) * 128, 128), span)

    def copy_to(k):
        peer = lax.rem(me + k, n)
        peer_g, peer_o = lax.div(peer, n_o), lax.rem(peer, n_o)
        return pltpu.make_async_remote_copy(
            src_ref=stage.at[:, window(peer_o)],
            dst_ref=recv.at[me],
            send_sem=send_sem.at[k],
            recv_sem=recv_sem.at[me],
            device_id=(peer_g, peer_o),
            device_id_type=MESH,
        )

    def copy_from(k):
        src = lax.rem(me + k, n)
        return pltpu.make_async_remote_copy(
            src_ref=stage.at[:, window(me_o)],
            dst_ref=recv.at[src],
            send_sem=send_sem.at[k],
            recv_sem=recv_sem.at[src],
            device_id=(lax.div(src, n_o), lax.rem(src, n_o)),
            device_id_type=MESH,
        )

    pl.semaphore_wait(barrier, n - 1)

    def send(k, carry):
        copy_to(k).start()
        return carry

    lax.fori_loop(1, n, send, 0)
    recv[me] = stage[:, window(me_o)]

    offset = lax.rem(me_o * cap, 128)
    first_col = me_g * quarter - REACH

    def onehots(points):
        index = points[0:1].astype(jnp.int32)
        place = lax.broadcasted_iota(jnp.int32, (1, span), 1) - offset
        reach = (index & (W - 1)) - first_col
        used = (place >= 0) & (place < cap) & (reach >= 0) & (reach < quarter + 2 * REACH)
        mass = jnp.where(used, points[1:2], 0.0)
        cell = (reach // LANES) * STRIP + index // W
        lane = reach & (LANES - 1)
        cell_iota = lax.broadcasted_iota(jnp.int32, (acc.shape[0], span), 0)
        lane_iota = lax.broadcasted_iota(jnp.int32, (LANES, span), 0)
        cells = jnp.where(cell_iota == cell, 1.0, 0.0).astype(jnp.bfloat16)
        lanes = jnp.where(lane_iota == lane, mass, 0.0).astype(jnp.bfloat16)
        return cells, lanes

    def bin_batch(t, carry):
        cells, lanes = [], []
        for u in range(BATCH):
            k = t * BATCH + u

            @pl.when(k > 0)
            def _():
                copy_from(k).wait_recv()

        for u in range(BATCH):
            a, b = onehots(recv[lax.rem(me + t * BATCH + u, n)])
            cells.append(a)
            lanes.append(b)
        acc[...] += lax.dot_general(
            jnp.concatenate(cells, axis=1),
            jnp.concatenate(lanes, axis=1),
            (((1,), (1,)), ((), ())),
            preferred_element_type=jnp.float32,
        )
        return carry

    lax.fori_loop(0, n // BATCH, bin_batch, 0)

    for t in range(tiles):
        at = pl.ds(t * LANES, LANES)
        heat = acc[t * STRIP : (t + 1) * STRIP, :]
        halo_out[0, :, at] = heat[STRIP - REACH :].astype(jnp.bfloat16)
        halo_out[1, :, at] = heat[:REACH].astype(jnp.bfloat16)
        ext[REACH : REACH + STRIP, at] = heat

    def halo_copy(side, owner):
        return pltpu.make_async_remote_copy(
            src_ref=halo_out.at[side],
            dst_ref=halo_in.at[side],
            send_sem=halo_send_sem.at[side],
            recv_sem=halo_recv_sem.at[side],
            device_id=(me_g, owner),
            device_id_type=MESH,
        )

    @pl.when(me_o < n_o - 1)
    def _():
        halo_copy(0, me_o + 1).start()

    @pl.when(me_o > 0)
    def _():
        halo_copy(1, me_o - 1).start()

    def sent(k, carry):
        copy_to(k).wait_send()
        return carry

    lax.fori_loop(1, n, sent, 0)

    @pl.when(me_o > 0)
    def _():
        halo_copy(0, me_o - 1).wait_recv()

    @pl.when(me_o < n_o - 1)
    def _():
        halo_copy(1, me_o + 1).wait_recv()

    ext[0:REACH, :] = halo_in[0].astype(jnp.float32)
    ext[REACH + STRIP :, :] = halo_in[1].astype(jnp.float32)

    def smooth(j, carry):
        start = pl.multiple_of(j * CHUNK, 128)
        rows = [ext[a : a + STRIP, pl.ds(start, CHUNK + 128)] for a in range(TAPS)]
        total = None
        for b in range(TAPS):
            part = rows[0] * kern_ref[0, b]
            for a in range(1, TAPS):
                part = part + rows[a] * kern_ref[a, b]
            part = part[:, b : b + CHUNK]
            total = part if total is None else total + part
        out_ref[:, pl.ds(start, CHUNK)] = total
        return carry

    lax.fori_loop(0, quarter // CHUNK, smooth, 0)

    @pl.when(me_o < n_o - 1)
    def _():
        halo_copy(0, me_o + 1).wait_send()

    @pl.when(me_o > 0)
    def _():
        halo_copy(1, me_o - 1).wait_send()


def per_device(tile_row, pixel_col, weight, counts, kernel):
    n_o = lax.axis_size("own")
    n_g = lax.axis_size("grp")
    n = n_g * n_o
    slots = tile_row.shape[2]
    cap = slots // n_o
    quarter = W // n_g
    span = -(-(max(o * cap % 128 for o in range(n_o)) + cap) // 128) * 128
    tiles = -(-(quarter + 2 * REACH) // LANES)
    width = tiles * LANES
    vmem = pl.BlockSpec(memory_space=pltpu.VMEM)
    smem = pl.BlockSpec(memory_space=pltpu.SMEM)
    return pl.pallas_call(
        functools.partial(heat_kernel, n_g, n_o, cap, span),
        out_shape=jax.ShapeDtypeStruct((STRIP, quarter), jnp.float32),
        in_specs=[vmem, vmem, vmem, smem, smem],
        out_specs=vmem,
        scratch_shapes=[
            pltpu.VMEM((2, slots), jnp.float32),
            pltpu.VMEM((n, 2, span), jnp.float32),
            pltpu.VMEM((tiles * STRIP, LANES), jnp.float32),
            pltpu.VMEM((2, REACH, width), jnp.bfloat16),
            pltpu.VMEM((2, REACH, width), jnp.bfloat16),
            pltpu.VMEM((STRIP + 2 * REACH, width), jnp.float32),
            pltpu.SemaphoreType.DMA((n,)),
            pltpu.SemaphoreType.DMA((n,)),
            pltpu.SemaphoreType.DMA((2,)),
            pltpu.SemaphoreType.DMA((2,)),
        ],
        compiler_params=pltpu.CompilerParams(collective_id=0, has_side_effects=True),
    )(tile_row, pixel_col, weight, counts, kernel)


def solution(mesh):
    placed = (
        P("grp", "own", None),
        P("grp", "own", None),
        P("grp", "own", None),
        P("grp", "own", None),
        P(),
    )
    return jax.shard_map(
        per_device, mesh=mesh, in_specs=placed, out_specs=P("own", "grp"), check_vma=False
    )
```

```python
import functools
import math

import jax
import jax.numpy as jnp
from jax import lax
from jax.experimental import pallas as pl
from jax.experimental.pallas import tpu as pltpu
from jax.sharding import PartitionSpec as P

W = 16384
STRIP = 8
REACH = 4
TAPS = 9
LANES = 256
CHUNK = 512
BATCH = 4
MESH = pl.DeviceIdType.MESH


def heat_kernel(
    n_g, n_o, cap, span, row_hbm, col_hbm, weight_hbm, counts_hbm, kern_hbm, out_ref,
    row_ref, col_ref, weight_ref, counts_ref, kern_ref,
    stage, recv, acc, halo_out, halo_in, ext, edge, edge_taps,
    load_sem, send_sem, recv_sem, halo_send_sem, halo_recv_sem,
):
    n = n_g * n_o
    me_g, me_o = lax.axis_index("grp"), lax.axis_index("own")
    me = me_g * n_o + me_o
    quarter = out_ref.shape[1]
    slots = row_ref.shape[2]
    tiles = acc.shape[0] // STRIP

    loads = [
        pltpu.make_async_copy(source, target, load_sem.at[k])
        for k, (source, target) in enumerate(
            [
                (row_hbm, row_ref),
                (col_hbm, col_ref),
                (weight_hbm, weight_ref),
                (counts_hbm, counts_ref),
                (kern_hbm, kern_ref),
            ]
        )
    ]
    for load in loads:
        load.start()

    barrier = pltpu.get_barrier_semaphore()

    def greet(k, carry):
        peer = lax.rem(me + k, n)
        pl.semaphore_signal(
            barrier, inc=1, device_id=(lax.div(peer, n_o), lax.rem(peer, n_o)), device_id_type=MESH
        )
        return carry

    lax.fori_loop(1, n, greet, 0)

    for load in loads:
        load.wait()

    period = math.lcm(cap, 128)
    per = period // cap

    def prepare(k, carry):
        at = pl.ds(pl.multiple_of(k * period, 128), period)
        lane = lax.broadcasted_iota(jnp.int32, (1, period), 1)
        limit = jnp.full((1, period), counts_ref[0, 0, k * per], jnp.int32)
        for j in range(1, per):
            limit = jnp.where(lane >= j * cap, counts_ref[0, 0, k * per + j] + j * cap, limit)
        index = row_ref[0, :, at] * W + col_ref[0, :, at]
        stage[0:1, at] = index.astype(jnp.float32)
        stage[1:2, at] = jnp.where(lane < limit, weight_ref[0, :, at].astype(jnp.float32), 0.0)
        return carry

    lax.fori_loop(0, slots // period, prepare, 0)
    for k in range(halo_in.shape[0]):
        halo_in_zero = jnp.zeros(halo_in.shape[1:], halo_in.dtype)

        @pl.when(me_o == (0 if k == 0 else n_o - 1))
        def _():
            halo_in[k] = halo_in_zero

    acc[...] = jnp.zeros_like(acc)
    ext[...] = jnp.zeros_like(ext)
    edge[...] = jnp.zeros_like(edge)
    upper = lax.broadcasted_iota(jnp.int32, (STRIP, 128), 0) < REACH
    for a in range(REACH):
        for b in range(TAPS):
            edge_taps[a * TAPS + b] = jnp.where(upper, kern_ref[a, b], kern_ref[a + REACH + 1, b])

    def partner(t):
        if n_o & (n_o - 1):
            return lax.rem(me_o + t, n_o)
        place, bit = 0, 1
        while bit < n_o:
            place = place + bit * lax.rem(lax.div(me_o, bit) + lax.div(t, bit), 2)
            bit *= 2
        return place

    def peer_of(k):
        return lax.rem(me_g + lax.rem(k, n_g), n_g), partner(lax.div(k, n_g))

    def source_of(k):
        return lax.rem(me_g + lax.rem(k, n_g), n_g), partner(lax.div(k, n_g))

    def window(owner):
        return pl.ds(pl.multiple_of(lax.div(owner * cap, 128) * 128, 128), span)

    def copy_to(k):
        peer_g, peer_o = peer_of(k)
        return pltpu.make_async_remote_copy(
            src_ref=stage.at[:, window(peer_o)],
            dst_ref=recv.at[me],
            send_sem=send_sem.at[k],
            recv_sem=recv_sem.at[me],
            device_id=(peer_g, peer_o),
            device_id_type=MESH,
        )

    def copy_from(k):
        src_g, src_o = source_of(k)
        src = src_g * n_o + src_o
        return pltpu.make_async_remote_copy(
            src_ref=stage.at[:, window(me_o)],
            dst_ref=recv.at[src],
            send_sem=send_sem.at[k],
            recv_sem=recv_sem.at[src],
            device_id=(src_g, src_o),
            device_id_type=MESH,
        )

    pl.semaphore_wait(barrier, n - 1)

    def send(k, carry):
        copy_to(k).start()
        return carry

    lax.fori_loop(1, n, send, 0)
    recv[me] = stage[:, window(me_o)]

    offset = lax.rem(me_o * cap, 128)
    first_col = me_g * quarter - REACH

    def onehots(points):
        index = points[0:1].astype(jnp.int32)
        place = lax.broadcasted_iota(jnp.int32, (1, span), 1) - offset
        reach = (index & (W - 1)) - first_col
        used = (place >= 0) & (place < cap) & (reach >= 0) & (reach < quarter + 2 * REACH)
        mass = jnp.where(used, points[1:2], 0.0)
        cell = (reach // LANES) * STRIP + index // W
        lane = reach & (LANES - 1)
        cell_iota = lax.broadcasted_iota(jnp.int32, (acc.shape[0], span), 0)
        lane_iota = lax.broadcasted_iota(jnp.int32, (LANES, span), 0)
        cells = jnp.where(cell_iota == cell, 1.0, 0.0).astype(jnp.bfloat16)
        lanes = jnp.where(lane_iota == lane, mass, 0.0).astype(jnp.bfloat16)
        return cells, lanes

    def bin_batch(t, carry):
        cells, lanes = [], []
        for u in range(BATCH):
            k = t * BATCH + u

            @pl.when(k > 0)
            def _():
                copy_from(k).wait_recv()

        for u in range(BATCH):
            src_g, src_o = source_of(t * BATCH + u)
            a, b = onehots(recv[src_g * n_o + src_o])
            cells.append(a)
            lanes.append(b)
        acc[...] += lax.dot_general(
            jnp.concatenate(cells, axis=1),
            jnp.concatenate(lanes, axis=1),
            (((1,), (1,)), ((), ())),
            preferred_element_type=jnp.float32,
        )
        return carry

    lax.fori_loop(0, n // BATCH, bin_batch, 0)

    for t in range(tiles):
        at = pl.ds(t * LANES, LANES)
        heat = acc[t * STRIP : (t + 1) * STRIP, :]
        halo_out[0, :, at] = heat[STRIP - REACH :].astype(jnp.bfloat16)
        halo_out[1, :, at] = heat[:REACH].astype(jnp.bfloat16)
        ext[REACH : REACH + STRIP, at] = heat

    def halo_copy(side, owner):
        return pltpu.make_async_remote_copy(
            src_ref=halo_out.at[side],
            dst_ref=halo_in.at[side],
            send_sem=halo_send_sem.at[side],
            recv_sem=halo_recv_sem.at[side],
            device_id=(me_g, owner),
            device_id_type=MESH,
        )

    @pl.when(me_o < n_o - 1)
    def _():
        halo_copy(0, me_o + 1).start()

    @pl.when(me_o > 0)
    def _():
        halo_copy(1, me_o - 1).start()

    def sent(k, carry):
        copy_to(k).wait_send()
        return carry

    lax.fori_loop(1, n, sent, 0)

    def smooth(j, carry):
        start = pl.multiple_of(j * CHUNK, 128)
        rows = [ext[a : a + STRIP, pl.ds(start, CHUNK + 128)] for a in range(TAPS)]
        total = None
        for b in range(TAPS):
            part = rows[0] * kern_ref[0, b]
            for a in range(1, TAPS):
                part = part + rows[a] * kern_ref[a, b]
            part = part[:, b : b + CHUNK]
            total = part if total is None else total + part
        out_ref[:, pl.ds(start, CHUNK)] = total
        return carry

    lax.fori_loop(0, quarter // CHUNK, smooth, 0)

    @pl.when(me_o > 0)
    def _():
        halo_copy(0, me_o - 1).wait_recv()

    @pl.when(me_o < n_o - 1)
    def _():
        halo_copy(1, me_o + 1).wait_recv()

    edge[0:REACH, :] = halo_in[0].astype(jnp.float32)
    edge[STRIP - 1 : STRIP - 1 + REACH, :] = halo_in[1].astype(jnp.float32)

    def smooth_edge(j, carry):
        start = pl.multiple_of(j * CHUNK, 128)
        rows = [edge[a : a + STRIP, pl.ds(start, CHUNK + 128)] for a in range(REACH)]
        total = out_ref[:, pl.ds(start, CHUNK)]
        for b in range(TAPS):
            part = None
            for a in range(REACH):
                taps = jnp.concatenate([edge_taps[a * TAPS + b]] * (CHUNK // 128 + 1), axis=1)
                term = rows[a] * taps
                part = term if part is None else part + term
            total = total + part[:, b : b + CHUNK]
        out_ref[:, pl.ds(start, CHUNK)] = total
        return carry

    lax.fori_loop(0, quarter // CHUNK, smooth_edge, 0)

    @pl.when(me_o < n_o - 1)
    def _():
        halo_copy(0, me_o + 1).wait_send()

    @pl.when(me_o > 0)
    def _():
        halo_copy(1, me_o - 1).wait_send()


def per_device(tile_row, pixel_col, weight, counts, kernel):
    n_o = lax.axis_size("own")
    n_g = lax.axis_size("grp")
    n = n_g * n_o
    slots = tile_row.shape[2]
    cap = slots // n_o
    quarter = W // n_g
    span = -(-(max(o * cap % 128 for o in range(n_o)) + cap) // 128) * 128
    tiles = -(-(quarter + 2 * REACH) // LANES)
    width = tiles * LANES
    vmem = pl.BlockSpec(memory_space=pltpu.VMEM)
    hbm = pl.BlockSpec(memory_space=pltpu.HBM)
    return pl.pallas_call(
        functools.partial(heat_kernel, n_g, n_o, cap, span),
        out_shape=pltpu.VMEM((STRIP, quarter), jnp.float32),
        in_specs=[hbm] * 5,
        out_specs=vmem,
        scratch_shapes=[
            pltpu.VMEM(tile_row.shape, jnp.int32),
            pltpu.VMEM(pixel_col.shape, jnp.int32),
            pltpu.VMEM(weight.shape, weight.dtype),
            pltpu.SMEM(counts.shape, jnp.int32),
            pltpu.SMEM(kernel.shape, jnp.float32),
            pltpu.VMEM((2, slots), jnp.float32),
            pltpu.VMEM((n, 2, span), jnp.float32),
            pltpu.VMEM((tiles * STRIP, LANES), jnp.float32),
            pltpu.VMEM((2, REACH, width), jnp.bfloat16),
            pltpu.VMEM((2, REACH, width), jnp.bfloat16),
            pltpu.VMEM((STRIP + 2 * REACH, width), jnp.float32),
            pltpu.VMEM((STRIP + 2 * REACH, width), jnp.float32),
            pltpu.VMEM((REACH * TAPS, STRIP, 128), jnp.float32),
            pltpu.SemaphoreType.DMA((5,)),
            pltpu.SemaphoreType.DMA((n,)),
            pltpu.SemaphoreType.DMA((n,)),
            pltpu.SemaphoreType.DMA((2,)),
            pltpu.SemaphoreType.DMA((2,)),
        ],
        compiler_params=pltpu.CompilerParams(collective_id=0, has_side_effects=True),
    )(tile_row, pixel_col, weight, counts, kernel)


def solution(mesh):
    placed = (
        P("grp", "own", None),
        P("grp", "own", None),
        P("grp", "own", None),
        P("grp", "own", None),
        P(),
    )
    return jax.shard_map(
        per_device, mesh=mesh, in_specs=placed, out_specs=P("own", "grp"), check_vma=False
    )
```

```python
import functools
import math

import jax
import jax.numpy as jnp
from jax import lax
from jax.experimental import pallas as pl
from jax.experimental.pallas import tpu as pltpu
from jax.sharding import PartitionSpec as P

W = 16384
STRIP = 8
REACH = 4
TAPS = 9
LANES = 256
CHUNK = 512
MESH = pl.DeviceIdType.MESH


def heat_kernel(
    n_g, n_o, cap, span, row_hbm, col_hbm, weight_hbm, counts_hbm, kern_hbm, out_ref,
    row_ref, col_ref, weight_ref, counts_ref, kern_ref,
    stage, recv, acc, halo_out, halo_in, own_rows, edge_rows, edge_taps,
    load_sem, send_sem, recv_sem, halo_send_sem, halo_recv_sem,
):
    n = n_g * n_o
    me_g, me_o = lax.axis_index("grp"), lax.axis_index("own")
    quarter = out_ref.shape[1]
    slots = row_ref.shape[2]
    tiles = acc.shape[0] // STRIP

    loads = [
        pltpu.make_async_copy(source, target, load_sem.at[k])
        for k, (source, target) in enumerate(
            [
                (row_hbm, row_ref),
                (col_hbm, col_ref),
                (weight_hbm, weight_ref),
                (counts_hbm, counts_ref),
                (kern_hbm, kern_ref),
            ]
        )
    ]
    for load in loads:
        load.start()

    barrier = pltpu.get_barrier_semaphore()

    def offset_place(mine, step, count):
        if count & (count - 1):
            return lax.rem(mine + step, count)
        place, bit = 0, 1
        while bit < count:
            place = place + bit * lax.rem(lax.div(mine, bit) + lax.div(step, bit), 2)
            bit *= 2
        return place

    def mirrored(step, count):
        return lax.rem(count - step, count) if count & (count - 1) else step

    groups = [offset_place(me_g, jnp.int32(u), n_g) for u in range(n_g)]

    def farthest_first(act):
        def ring(r, carry):
            step = n_o - 1 - r
            owner = offset_place(me_o, step, n_o)
            for u in range(n_g):
                act(step, u, owner)
            return carry

        lax.fori_loop(0, n_o - 1, ring, 0)
        for u in range(1, n_g):
            act(0, u, me_o)

    farthest_first(
        lambda step, u, owner: pl.semaphore_signal(
            barrier, inc=1, device_id=(groups[u], owner), device_id_type=MESH
        )
    )

    for load in loads:
        load.wait()

    period = math.lcm(cap, 128)
    per = period // cap

    def prepare(k, carry):
        at = pl.ds(pl.multiple_of(k * period, 128), period)
        lane = lax.broadcasted_iota(jnp.int32, (1, period), 1)
        limit = jnp.full((1, period), counts_ref[0, 0, k * per], jnp.int32)
        for j in range(1, per):
            limit = jnp.where(lane >= j * cap, counts_ref[0, 0, k * per + j] + j * cap, limit)
        index = row_ref[0, :, at] * W + col_ref[0, :, at]
        stage[0:1, at] = index.astype(jnp.float32)
        stage[1:2, at] = jnp.where(lane < limit, weight_ref[0, :, at].astype(jnp.float32), 0.0)
        return carry

    lax.fori_loop(0, slots // period, prepare, 0)
    for k in range(halo_in.shape[0]):
        halo_in_zero = jnp.zeros(halo_in.shape[1:], halo_in.dtype)

        @pl.when(me_o == (0 if k == 0 else n_o - 1))
        def _():
            halo_in[k] = halo_in_zero

    acc[...] = jnp.zeros_like(acc)
    upper = lax.broadcasted_iota(jnp.int32, (STRIP, 128), 0) < REACH
    for a in range(REACH):
        for b in range(TAPS):
            edge_taps[a * TAPS + b] = jnp.where(upper, kern_ref[a, b], kern_ref[a + REACH + 1, b])

    def window(owner):
        return pl.ds(pl.multiple_of(lax.div(owner * cap, 128) * 128, 128), span)

    def copy(step, u, owner):
        there = mirrored(step, n_o) * n_g + mirrored(u, n_g)
        return pltpu.make_async_remote_copy(
            src_ref=stage.at[:, window(owner)],
            dst_ref=recv.at[there],
            send_sem=send_sem.at[step * n_g + u],
            recv_sem=recv_sem.at[there],
            device_id=(groups[u], owner),
            device_id_type=MESH,
        )

    def arrival(k):
        return pltpu.make_async_remote_copy(
            src_ref=recv.at[k],
            dst_ref=recv.at[k],
            send_sem=send_sem.at[k],
            recv_sem=recv_sem.at[k],
            device_id=(me_g, me_o),
            device_id_type=MESH,
        )

    pl.semaphore_wait(barrier, n - 1)

    farthest_first(lambda step, u, owner: copy(step, u, owner).start())
    recv[0] = stage[:, window(me_o)]

    offset = lax.rem(me_o * cap, 128)
    first_col = me_g * quarter - REACH

    def onehots(points):
        index = points[0:1].astype(jnp.int32)
        place = lax.broadcasted_iota(jnp.int32, (1, span), 1) - offset
        reach = (index & (W - 1)) - first_col
        used = (place >= 0) & (place < cap) & (reach >= 0) & (reach < quarter + 2 * REACH)
        mass = jnp.where(used, points[1:2], 0.0)
        cell = (reach // LANES) * STRIP + index // W
        lane = reach & (LANES - 1)
        cell_iota = lax.broadcasted_iota(jnp.int32, (acc.shape[0], span), 0)
        lane_iota = lax.broadcasted_iota(jnp.int32, (LANES, span), 0)
        cells = jnp.where(cell_iota == cell, 1.0, 0.0).astype(jnp.bfloat16)
        lanes = jnp.where(lane_iota == lane, mass, 0.0).astype(jnp.bfloat16)
        return cells, lanes

    def bin_batch(t, carry):
        cells, lanes = [], []
        for u in range(n_g):
            if u == 0:

                @pl.when(t > 0)
                def _():
                    arrival(t * n_g).wait_recv()
            else:
                arrival(t * n_g + u).wait_recv()
        for u in range(n_g):
            a, b = onehots(recv[t * n_g + u])
            cells.append(a)
            lanes.append(b)
        acc[...] += lax.dot_general(
            jnp.concatenate(cells, axis=1),
            jnp.concatenate(lanes, axis=1),
            (((1,), (1,)), ((), ())),
            preferred_element_type=jnp.float32,
        )
        return carry

    lax.fori_loop(0, n_o, bin_batch, 0)

    for t in range(tiles):
        at = pl.ds(t * LANES, LANES)
        heat = acc[t * STRIP : (t + 1) * STRIP, :]
        halo_out[0, :, at] = heat[STRIP - REACH :].astype(jnp.bfloat16)
        halo_out[1, :, at] = heat[:REACH].astype(jnp.bfloat16)

    def halo_copy(side, owner):
        return pltpu.make_async_remote_copy(
            src_ref=halo_out.at[side],
            dst_ref=halo_in.at[side],
            send_sem=halo_send_sem.at[side],
            recv_sem=halo_recv_sem.at[side],
            device_id=(me_g, owner),
            device_id_type=MESH,
        )

    @pl.when(me_o < n_o - 1)
    def _():
        halo_copy(0, me_o + 1).start()

    @pl.when(me_o > 0)
    def _():
        halo_copy(1, me_o - 1).start()

    def sent(k, carry):
        arrival(k).wait_send()
        return carry

    lax.fori_loop(1, n, sent, 0)

    blank = jnp.zeros((REACH, LANES), jnp.float32)

    def shift_own(t, carry):
        heat = acc[pl.ds(pl.multiple_of(t * STRIP, STRIP), STRIP), :]
        framed = jnp.concatenate([blank, heat, blank], axis=0)
        for a in range(TAPS):
            own_rows[a, :, pl.ds(pl.multiple_of(t * LANES, LANES), LANES)] = framed[a : a + STRIP]
        return carry

    lax.fori_loop(0, tiles, shift_own, 0)

    def smooth(j, carry):
        start = pl.multiple_of(j * CHUNK, 128)
        rows = [own_rows[a, :, pl.ds(start, CHUNK + 128)] for a in range(TAPS)]
        total = None
        for b in range(TAPS):
            part = rows[0] * kern_ref[0, b]
            for a in range(1, TAPS):
                part = part + rows[a] * kern_ref[a, b]
            part = part[:, b : b + CHUNK]
            total = part if total is None else total + part
        out_ref[:, pl.ds(start, CHUNK)] = total
        return carry

    lax.fori_loop(0, quarter // CHUNK, smooth, 0)

    @pl.when(me_o > 0)
    def _():
        halo_copy(0, me_o - 1).wait_recv()

    @pl.when(me_o < n_o - 1)
    def _():
        halo_copy(1, me_o + 1).wait_recv()

    def shift_edge(t, carry):
        at = pl.ds(pl.multiple_of(t * LANES, LANES), LANES)
        above = halo_in[0, :, at].astype(jnp.float32)
        below = halo_in[1, :, at].astype(jnp.float32)
        framed = jnp.concatenate([above, blank[: REACH - 1], below], axis=0)
        for a in range(REACH):
            edge_rows[a, :, at] = framed[a : a + STRIP]
        return carry

    lax.fori_loop(0, tiles, shift_edge, 0)

    def smooth_edge(j, carry):
        start = pl.multiple_of(j * CHUNK, 128)
        rows = [edge_rows[a, :, pl.ds(start, CHUNK + 128)] for a in range(REACH)]
        total = out_ref[:, pl.ds(start, CHUNK)]
        for b in range(TAPS):
            part = None
            for a in range(REACH):
                taps = jnp.concatenate([edge_taps[a * TAPS + b]] * (CHUNK // 128 + 1), axis=1)
                term = rows[a] * taps
                part = term if part is None else part + term
            total = total + part[:, b : b + CHUNK]
        out_ref[:, pl.ds(start, CHUNK)] = total
        return carry

    lax.fori_loop(0, quarter // CHUNK, smooth_edge, 0)

    @pl.when(me_o < n_o - 1)
    def _():
        halo_copy(0, me_o + 1).wait_send()

    @pl.when(me_o > 0)
    def _():
        halo_copy(1, me_o - 1).wait_send()


def per_device(tile_row, pixel_col, weight, counts, kernel):
    n_o = lax.axis_size("own")
    n_g = lax.axis_size("grp")
    n = n_g * n_o
    slots = tile_row.shape[2]
    cap = slots // n_o
    quarter = W // n_g
    span = -(-(max(o * cap % 128 for o in range(n_o)) + cap) // 128) * 128
    tiles = -(-(quarter + 2 * REACH) // LANES)
    width = tiles * LANES
    vmem = pl.BlockSpec(memory_space=pltpu.VMEM)
    hbm = pl.BlockSpec(memory_space=pltpu.HBM)
    return pl.pallas_call(
        functools.partial(heat_kernel, n_g, n_o, cap, span),
        out_shape=pltpu.VMEM((STRIP, quarter), jnp.float32),
        in_specs=[hbm] * 5,
        out_specs=vmem,
        scratch_shapes=[
            pltpu.VMEM(tile_row.shape, jnp.int32),
            pltpu.VMEM(pixel_col.shape, jnp.int32),
            pltpu.VMEM(weight.shape, weight.dtype),
            pltpu.SMEM(counts.shape, jnp.int32),
            pltpu.SMEM(kernel.shape, jnp.float32),
            pltpu.VMEM((2, slots), jnp.float32),
            pltpu.VMEM((n, 2, span), jnp.float32),
            pltpu.VMEM((tiles * STRIP, LANES), jnp.float32),
            pltpu.VMEM((2, REACH, width), jnp.bfloat16),
            pltpu.VMEM((2, REACH, width), jnp.bfloat16),
            pltpu.VMEM((TAPS, STRIP, width), jnp.float32),
            pltpu.VMEM((REACH, STRIP, width), jnp.float32),
            pltpu.VMEM((REACH * TAPS, STRIP, 128), jnp.float32),
            pltpu.SemaphoreType.DMA((5,)),
            pltpu.SemaphoreType.DMA((n,)),
            pltpu.SemaphoreType.DMA((n,)),
            pltpu.SemaphoreType.DMA((2,)),
            pltpu.SemaphoreType.DMA((2,)),
        ],
        compiler_params=pltpu.CompilerParams(collective_id=0, has_side_effects=True),
    )(tile_row, pixel_col, weight, counts, kernel)


def solution(mesh):
    placed = (
        P("grp", "own", None),
        P("grp", "own", None),
        P("grp", "own", None),
        P("grp", "own", None),
        P(),
    )
    return jax.shard_map(
        per_device, mesh=mesh, in_specs=placed, out_specs=P("own", "grp"), check_vma=False
    )
```

```python
import functools
import math

import jax
import jax.numpy as jnp
from jax import lax
from jax.experimental import pallas as pl
from jax.experimental.pallas import tpu as pltpu
from jax.sharding import PartitionSpec as P

W = 16384
STRIP = 8
REACH = 4
TAPS = 9
LANES = 256
CHUNK = 512
MESH = pl.DeviceIdType.MESH


def heat_kernel(
    n_g, n_o, cap, span, row_hbm, col_hbm, weight_hbm, counts_hbm, kern_hbm, out_ref,
    row_ref, col_ref, weight_ref, counts_ref, kern_ref,
    stage, recv, acc, halo_out, halo_in, own_rows, edge_rows, edge_taps,
    load_sem, send_sem, recv_sem, halo_send_sem, halo_recv_sem,
):
    n = n_g * n_o
    me_g, me_o = lax.axis_index("grp"), lax.axis_index("own")
    quarter = out_ref.shape[1]
    slots = row_ref.shape[2]
    tiles = acc.shape[0] // STRIP

    loads = [
        pltpu.make_async_copy(source, target, load_sem.at[k])
        for k, (source, target) in enumerate(
            [
                (row_hbm, row_ref),
                (col_hbm, col_ref),
                (weight_hbm, weight_ref),
                (counts_hbm, counts_ref),
                (kern_hbm, kern_ref),
            ]
        )
    ]
    for load in loads:
        load.start()

    barrier = pltpu.get_barrier_semaphore()

    def offset_place(mine, step, count):
        if count & (count - 1):
            return lax.rem(mine + step, count)
        place, bit = 0, 1
        while bit < count:
            place = place + bit * lax.rem(lax.div(mine, bit) + lax.div(step, bit), 2)
            bit *= 2
        return place

    def mirrored(step, count):
        return lax.rem(count - step, count) if count & (count - 1) else step

    groups = [offset_place(me_g, jnp.int32(u), n_g) for u in range(n_g)]

    def farthest_first(act):
        def ring(r, carry):
            step = n_o - 1 - r
            owner = offset_place(me_o, step, n_o)
            for u in range(n_g):
                act(step, u, owner)
            return carry

        lax.fori_loop(0, n_o - 1, ring, 0)
        for u in range(1, n_g):
            act(0, u, me_o)

    farthest_first(
        lambda step, u, owner: pl.semaphore_signal(
            barrier, inc=1, device_id=(groups[u], owner), device_id_type=MESH
        )
    )

    for load in loads:
        load.wait()

    period = math.lcm(cap, 128)
    per = period // cap

    def prepare(k, carry):
        at = pl.ds(pl.multiple_of(k * period, 128), period)
        lane = lax.broadcasted_iota(jnp.int32, (1, period), 1)
        limit = jnp.full((1, period), counts_ref[0, 0, k * per], jnp.int32)
        for j in range(1, per):
            limit = jnp.where(lane >= j * cap, counts_ref[0, 0, k * per + j] + j * cap, limit)
        index = row_ref[0, :, at] * W + col_ref[0, :, at]
        stage[0:1, at] = index.astype(jnp.float32)
        stage[1:2, at] = jnp.where(lane < limit, weight_ref[0, :, at].astype(jnp.float32), 0.0)
        return carry

    lax.fori_loop(0, slots // period, prepare, 0)
    for k in range(halo_in.shape[0]):
        halo_in_zero = jnp.zeros(halo_in.shape[1:], halo_in.dtype)

        @pl.when(me_o == (0 if k == 0 else n_o - 1))
        def _():
            halo_in[k] = halo_in_zero

    acc[...] = jnp.zeros_like(acc)
    upper = lax.broadcasted_iota(jnp.int32, (STRIP, 128), 0) < REACH
    for a in range(REACH):
        for b in range(TAPS):
            edge_taps[a * TAPS + b] = jnp.where(upper, kern_ref[a, b], kern_ref[a + REACH + 1, b])

    def window(owner):
        return pl.ds(pl.multiple_of(lax.div(owner * cap, 128) * 128, 128), span)

    def copy(step, u, owner):
        there = mirrored(step, n_o) * n_g + mirrored(u, n_g)
        return pltpu.make_async_remote_copy(
            src_ref=stage.at[:, window(owner)],
            dst_ref=recv.at[there],
            send_sem=send_sem.at[step * n_g + u],
            recv_sem=recv_sem.at[there],
            device_id=(groups[u], owner),
            device_id_type=MESH,
        )

    def arrival(k):
        return pltpu.make_async_remote_copy(
            src_ref=recv.at[k],
            dst_ref=recv.at[k],
            send_sem=send_sem.at[k],
            recv_sem=recv_sem.at[k],
            device_id=(me_g, me_o),
            device_id_type=MESH,
        )

    pl.semaphore_wait(barrier, n - 1)

    farthest_first(lambda step, u, owner: copy(step, u, owner).start())
    recv[0] = stage[:, window(me_o)]

    offset = lax.rem(me_o * cap, 128)
    first_col = me_g * quarter - REACH

    def onehots(points):
        index = points[0:1].astype(jnp.int32)
        place = lax.broadcasted_iota(jnp.int32, (1, span), 1) - offset
        reach = (index & (W - 1)) - first_col
        used = (place >= 0) & (place < cap) & (reach >= 0) & (reach < quarter + 2 * REACH)
        mass = jnp.where(used, points[1:2], 0.0)
        cell = (reach // LANES) * STRIP + index // W
        lane = reach & (LANES - 1)
        half = jnp.bfloat16
        cell = jnp.where(used, cell, 0).astype(jnp.float32).astype(half)
        lane = lane.astype(jnp.float32).astype(half)
        cell_iota = lax.broadcasted_iota(jnp.int32, (acc.shape[0], span), 0).astype(jnp.float32).astype(half)
        lane_iota = lax.broadcasted_iota(jnp.int32, (LANES, span), 0).astype(jnp.float32).astype(half)
        cells = jnp.where(cell_iota == cell, half(1), half(0))
        lanes = jnp.where(lane_iota == lane, mass.astype(half), half(0))
        return cells, lanes

    def bin_batch(t, carry):
        cells, lanes = [], []
        for u in range(n_g):
            if u == 0:

                @pl.when(t > 0)
                def _():
                    arrival(t * n_g).wait_recv()
            else:
                arrival(t * n_g + u).wait_recv()
        for u in range(n_g):
            a, b = onehots(recv[t * n_g + u])
            cells.append(a)
            lanes.append(b)
        acc[...] += lax.dot_general(
            jnp.concatenate(cells, axis=1),
            jnp.concatenate(lanes, axis=1),
            (((1,), (1,)), ((), ())),
            preferred_element_type=jnp.float32,
        )
        return carry

    lax.fori_loop(0, n_o, bin_batch, 0)

    for t in range(tiles):
        at = pl.ds(t * LANES, LANES)
        heat = acc[t * STRIP : (t + 1) * STRIP, :]
        halo_out[0, :, at] = heat[STRIP - REACH :].astype(jnp.bfloat16)
        halo_out[1, :, at] = heat[:REACH].astype(jnp.bfloat16)

    def halo_copy(side, owner):
        return pltpu.make_async_remote_copy(
            src_ref=halo_out.at[side],
            dst_ref=halo_in.at[side],
            send_sem=halo_send_sem.at[side],
            recv_sem=halo_recv_sem.at[side],
            device_id=(me_g, owner),
            device_id_type=MESH,
        )

    @pl.when(me_o < n_o - 1)
    def _():
        halo_copy(0, me_o + 1).start()

    @pl.when(me_o > 0)
    def _():
        halo_copy(1, me_o - 1).start()

    def sent(k, carry):
        arrival(k).wait_send()
        return carry

    lax.fori_loop(1, n, sent, 0)

    blank = jnp.zeros((REACH, LANES), jnp.float32)

    def shift_own(t, carry):
        heat = acc[pl.ds(pl.multiple_of(t * STRIP, STRIP), STRIP), :]
        framed = jnp.concatenate([blank, heat, blank], axis=0)
        for a in range(TAPS):
            own_rows[a, :, pl.ds(pl.multiple_of(t * LANES, LANES), LANES)] = framed[a : a + STRIP]
        return carry

    lax.fori_loop(0, tiles, shift_own, 0)

    def smooth(j, carry):
        start = pl.multiple_of(j * CHUNK, 128)
        rows = [own_rows[a, :, pl.ds(start, CHUNK + 128)] for a in range(TAPS)]
        total = None
        for b in range(TAPS):
            part = rows[0] * kern_ref[0, b]
            for a in range(1, TAPS):
                part = part + rows[a] * kern_ref[a, b]
            part = part[:, b : b + CHUNK]
            total = part if total is None else total + part
        out_ref[:, pl.ds(start, CHUNK)] = total
        return carry

    lax.fori_loop(0, quarter // CHUNK, smooth, 0)

    @pl.when(me_o > 0)
    def _():
        halo_copy(0, me_o - 1).wait_recv()

    @pl.when(me_o < n_o - 1)
    def _():
        halo_copy(1, me_o + 1).wait_recv()

    def shift_edge(t, carry):
        at = pl.ds(pl.multiple_of(t * LANES, LANES), LANES)
        above = halo_in[0, :, at].astype(jnp.float32)
        below = halo_in[1, :, at].astype(jnp.float32)
        framed = jnp.concatenate([above, blank[: REACH - 1], below], axis=0)
        for a in range(REACH):
            edge_rows[a, :, at] = framed[a : a + STRIP]
        return carry

    lax.fori_loop(0, tiles, shift_edge, 0)

    def smooth_edge(j, carry):
        start = pl.multiple_of(j * CHUNK, 128)
        rows = [edge_rows[a, :, pl.ds(start, CHUNK + 128)] for a in range(REACH)]
        total = out_ref[:, pl.ds(start, CHUNK)]
        for b in range(TAPS):
            part = None
            for a in range(REACH):
                taps = jnp.concatenate([edge_taps[a * TAPS + b]] * (CHUNK // 128 + 1), axis=1)
                term = rows[a] * taps
                part = term if part is None else part + term
            total = total + part[:, b : b + CHUNK]
        out_ref[:, pl.ds(start, CHUNK)] = total
        return carry

    lax.fori_loop(0, quarter // CHUNK, smooth_edge, 0)

    @pl.when(me_o < n_o - 1)
    def _():
        halo_copy(0, me_o + 1).wait_send()

    @pl.when(me_o > 0)
    def _():
        halo_copy(1, me_o - 1).wait_send()


def per_device(tile_row, pixel_col, weight, counts, kernel):
    n_o = lax.axis_size("own")
    n_g = lax.axis_size("grp")
    n = n_g * n_o
    slots = tile_row.shape[2]
    cap = slots // n_o
    quarter = W // n_g
    span = -(-(max(o * cap % 128 for o in range(n_o)) + cap) // 128) * 128
    tiles = -(-(quarter + 2 * REACH) // LANES)
    width = tiles * LANES
    vmem = pl.BlockSpec(memory_space=pltpu.VMEM)
    hbm = pl.BlockSpec(memory_space=pltpu.HBM)
    return pl.pallas_call(
        functools.partial(heat_kernel, n_g, n_o, cap, span),
        out_shape=pltpu.VMEM((STRIP, quarter), jnp.float32),
        in_specs=[hbm] * 5,
        out_specs=vmem,
        scratch_shapes=[
            pltpu.VMEM(tile_row.shape, jnp.int32),
            pltpu.VMEM(pixel_col.shape, jnp.int32),
            pltpu.VMEM(weight.shape, weight.dtype),
            pltpu.SMEM(counts.shape, jnp.int32),
            pltpu.SMEM(kernel.shape, jnp.float32),
            pltpu.VMEM((2, slots), jnp.float32),
            pltpu.VMEM((n, 2, span), jnp.float32),
            pltpu.VMEM((tiles * STRIP, LANES), jnp.float32),
            pltpu.VMEM((2, REACH, width), jnp.bfloat16),
            pltpu.VMEM((2, REACH, width), jnp.bfloat16),
            pltpu.VMEM((TAPS, STRIP, width), jnp.float32),
            pltpu.VMEM((REACH, STRIP, width), jnp.float32),
            pltpu.VMEM((REACH * TAPS, STRIP, 128), jnp.float32),
            pltpu.SemaphoreType.DMA((5,)),
            pltpu.SemaphoreType.DMA((n,)),
            pltpu.SemaphoreType.DMA((n,)),
            pltpu.SemaphoreType.DMA((2,)),
            pltpu.SemaphoreType.DMA((2,)),
        ],
        compiler_params=pltpu.CompilerParams(collective_id=0, has_side_effects=True),
    )(tile_row, pixel_col, weight, counts, kernel)


def solution(mesh):
    placed = (
        P("grp", "own", None),
        P("grp", "own", None),
        P("grp", "own", None),
        P("grp", "own", None),
        P(),
    )
    return jax.shard_map(
        per_device, mesh=mesh, in_specs=placed, out_specs=P("own", "grp"), check_vma=False
    )
```

```python
import functools
import math

import jax
import jax.numpy as jnp
from jax import lax
from jax.experimental import pallas as pl
from jax.experimental.pallas import tpu as pltpu
from jax.sharding import PartitionSpec as P

W = 16384
STRIP = 8
REACH = 4
TAPS = 9
LANES = 256
CHUNK = 1024
MESH = pl.DeviceIdType.MESH


def heat_kernel(
    n_g, n_o, cap, span, row_hbm, col_hbm, weight_hbm, counts_hbm, kern_hbm, out_ref,
    row_ref, col_ref, weight_ref, counts_ref, kern_ref,
    stage, recv, acc, halo_out, halo_in, own_rows, edge_rows, edge_taps,
    load_sem, send_sem, recv_sem, halo_send_sem, halo_recv_sem,
):
    n = n_g * n_o
    me_g, me_o = lax.axis_index("grp"), lax.axis_index("own")
    quarter = out_ref.shape[1]
    slots = row_ref.shape[2]
    tiles = acc.shape[0] // STRIP

    loads = [
        pltpu.make_async_copy(source, target, load_sem.at[k])
        for k, (source, target) in enumerate(
            [
                (row_hbm, row_ref),
                (col_hbm, col_ref),
                (weight_hbm, weight_ref),
                (counts_hbm, counts_ref),
                (kern_hbm, kern_ref),
            ]
        )
    ]
    for load in loads:
        load.start()

    barrier = pltpu.get_barrier_semaphore()

    def offset_place(mine, step, count):
        if count & (count - 1):
            return lax.rem(mine + step, count)
        place, bit = 0, 1
        while bit < count:
            place = place + bit * lax.rem(lax.div(mine, bit) + lax.div(step, bit), 2)
            bit *= 2
        return place

    def mirrored(step, count):
        return lax.rem(count - step, count) if count & (count - 1) else step

    groups = [offset_place(me_g, jnp.int32(u), n_g) for u in range(n_g)]

    def farthest_first(act):
        def ring(r, carry):
            step = n_o - 1 - r
            owner = offset_place(me_o, step, n_o)
            for u in reversed(range(n_g)):
                act(step, u, owner)
            return carry

        lax.fori_loop(0, n_o - 1, ring, 0)
        for u in range(1, n_g):
            act(0, u, me_o)

    farthest_first(
        lambda step, u, owner: pl.semaphore_signal(
            barrier, inc=1, device_id=(groups[u], owner), device_id_type=MESH
        )
    )

    for load in loads:
        load.wait()

    period = math.lcm(cap, 128)
    per = period // cap

    def prepare(k, carry):
        at = pl.ds(pl.multiple_of(k * period, 128), period)
        lane = lax.broadcasted_iota(jnp.int32, (1, period), 1)
        limit = jnp.full((1, period), counts_ref[0, 0, k * per], jnp.int32)
        for j in range(1, per):
            limit = jnp.where(lane >= j * cap, counts_ref[0, 0, k * per + j] + j * cap, limit)
        index = row_ref[0, :, at] * W + col_ref[0, :, at]
        stage[0:1, at] = index.astype(jnp.float32)
        stage[1:2, at] = jnp.where(lane < limit, weight_ref[0, :, at].astype(jnp.float32), 0.0)
        return carry

    lax.fori_loop(0, slots // period, prepare, 0)
    for k in range(halo_in.shape[0]):
        halo_in_zero = jnp.zeros(halo_in.shape[1:], halo_in.dtype)

        @pl.when(me_o == (0 if k == 0 else n_o - 1))
        def _():
            halo_in[k] = halo_in_zero

    acc[...] = jnp.zeros_like(acc)
    upper = lax.broadcasted_iota(jnp.int32, (STRIP, 128), 0) < REACH
    for a in range(REACH):
        for b in range(TAPS):
            edge_taps[a * TAPS + b] = jnp.where(upper, kern_ref[a, b], kern_ref[a + REACH + 1, b])

    def window(owner):
        return pl.ds(pl.multiple_of(lax.div(owner * cap, 128) * 128, 128), span)

    def copy(step, u, owner):
        there = mirrored(step, n_o) * n_g + mirrored(u, n_g)
        return pltpu.make_async_remote_copy(
            src_ref=stage.at[:, window(owner)],
            dst_ref=recv.at[there],
            send_sem=send_sem.at[step * n_g + u],
            recv_sem=recv_sem.at[there],
            device_id=(groups[u], owner),
            device_id_type=MESH,
        )

    def arrival(k):
        return pltpu.make_async_remote_copy(
            src_ref=recv.at[k],
            dst_ref=recv.at[k],
            send_sem=send_sem.at[k],
            recv_sem=recv_sem.at[k],
            device_id=(me_g, me_o),
            device_id_type=MESH,
        )

    pl.semaphore_wait(barrier, n - 1)

    farthest_first(lambda step, u, owner: copy(step, u, owner).start())
    recv[0] = stage[:, window(me_o)]

    offset = lax.rem(me_o * cap, 128)
    first_col = me_g * quarter - REACH

    def onehots(points):
        index = points[0:1].astype(jnp.int32)
        place = lax.broadcasted_iota(jnp.int32, (1, span), 1) - offset
        reach = (index & (W - 1)) - first_col
        used = (place >= 0) & (place < cap) & (reach >= 0) & (reach < quarter + 2 * REACH)
        mass = jnp.where(used, points[1:2], 0.0)
        cell = (reach // LANES) * STRIP + index // W
        lane = reach & (LANES - 1)
        half = jnp.bfloat16
        cell = jnp.where(used, cell, 0).astype(jnp.float32).astype(half)
        lane = lane.astype(jnp.float32).astype(half)
        cell_iota = lax.broadcasted_iota(jnp.int32, (acc.shape[0], span), 0).astype(jnp.float32).astype(half)
        lane_iota = lax.broadcasted_iota(jnp.int32, (LANES, span), 0).astype(jnp.float32).astype(half)
        cells = jnp.where(cell_iota == cell, half(1), half(0))
        lanes = jnp.where(lane_iota == lane, mass.astype(half), half(0))
        return cells, lanes

    def bin_batch(t, carry):
        cells, lanes = [], []
        for u in range(n_g):
            if u == 0:

                @pl.when(t > 0)
                def _():
                    arrival(t * n_g).wait_recv()
            else:
                arrival(t * n_g + u).wait_recv()
        for u in range(n_g):
            a, b = onehots(recv[t * n_g + u])
            cells.append(a)
            lanes.append(b)
        acc[...] += lax.dot_general(
            jnp.concatenate(cells, axis=1),
            jnp.concatenate(lanes, axis=1),
            (((1,), (1,)), ((), ())),
            preferred_element_type=jnp.float32,
        )
        return carry

    lax.fori_loop(0, n_o, bin_batch, 0)

    for t in range(tiles):
        at = pl.ds(t * LANES, LANES)
        heat = acc[t * STRIP : (t + 1) * STRIP, :]
        halo_out[0, :, at] = heat[STRIP - REACH :].astype(jnp.bfloat16)
        halo_out[1, :, at] = heat[:REACH].astype(jnp.bfloat16)

    def halo_copy(side, owner):
        return pltpu.make_async_remote_copy(
            src_ref=halo_out.at[side],
            dst_ref=halo_in.at[side],
            send_sem=halo_send_sem.at[side],
            recv_sem=halo_recv_sem.at[side],
            device_id=(me_g, owner),
            device_id_type=MESH,
        )

    @pl.when(me_o < n_o - 1)
    def _():
        halo_copy(0, me_o + 1).start()

    @pl.when(me_o > 0)
    def _():
        halo_copy(1, me_o - 1).start()

    def sent(k, carry):
        arrival(k).wait_send()
        return carry

    lax.fori_loop(1, n, sent, 0)

    blank = jnp.zeros((REACH, LANES), jnp.float32)

    def shift_own(t, carry):
        heat = acc[pl.ds(pl.multiple_of(t * STRIP, STRIP), STRIP), :]
        framed = jnp.concatenate([blank, heat, blank], axis=0)
        for a in range(TAPS):
            own_rows[a, :, pl.ds(pl.multiple_of(t * LANES, LANES), LANES)] = framed[a : a + STRIP]
        return carry

    lax.fori_loop(0, tiles, shift_own, 0)

    def smooth(j, carry):
        start = pl.multiple_of(j * CHUNK, 128)
        rows = [own_rows[a, :, pl.ds(start, CHUNK + 128)] for a in range(TAPS)]
        total = None
        for b in range(TAPS):
            part = rows[0] * kern_ref[0, b]
            for a in range(1, TAPS):
                part = part + rows[a] * kern_ref[a, b]
            part = part[:, b : b + CHUNK]
            total = part if total is None else total + part
        out_ref[:, pl.ds(start, CHUNK)] = total
        return carry

    lax.fori_loop(0, quarter // CHUNK, smooth, 0)

    @pl.when(me_o > 0)
    def _():
        halo_copy(0, me_o - 1).wait_recv()

    @pl.when(me_o < n_o - 1)
    def _():
        halo_copy(1, me_o + 1).wait_recv()

    def shift_edge(t, carry):
        at = pl.ds(pl.multiple_of(t * LANES, LANES), LANES)
        above = halo_in[0, :, at].astype(jnp.float32)
        below = halo_in[1, :, at].astype(jnp.float32)
        framed = jnp.concatenate([above, blank[: REACH - 1], below], axis=0)
        for a in range(REACH):
            edge_rows[a, :, at] = framed[a : a + STRIP]
        return carry

    lax.fori_loop(0, tiles, shift_edge, 0)

    def smooth_edge(j, carry):
        start = pl.multiple_of(j * CHUNK, 128)
        rows = [edge_rows[a, :, pl.ds(start, CHUNK + 128)] for a in range(REACH)]
        total = out_ref[:, pl.ds(start, CHUNK)]
        for b in range(TAPS):
            part = None
            for a in range(REACH):
                taps = jnp.concatenate([edge_taps[a * TAPS + b]] * (CHUNK // 128 + 1), axis=1)
                term = rows[a] * taps
                part = term if part is None else part + term
            total = total + part[:, b : b + CHUNK]
        out_ref[:, pl.ds(start, CHUNK)] = total
        return carry

    lax.fori_loop(0, quarter // CHUNK, smooth_edge, 0)

    @pl.when(me_o < n_o - 1)
    def _():
        halo_copy(0, me_o + 1).wait_send()

    @pl.when(me_o > 0)
    def _():
        halo_copy(1, me_o - 1).wait_send()


def per_device(tile_row, pixel_col, weight, counts, kernel):
    n_o = lax.axis_size("own")
    n_g = lax.axis_size("grp")
    n = n_g * n_o
    slots = tile_row.shape[2]
    cap = slots // n_o
    quarter = W // n_g
    span = -(-(max(o * cap % 128 for o in range(n_o)) + cap) // 128) * 128
    tiles = -(-(quarter + 2 * REACH) // LANES)
    width = tiles * LANES
    vmem = pl.BlockSpec(memory_space=pltpu.VMEM)
    hbm = pl.BlockSpec(memory_space=pltpu.HBM)
    return pl.pallas_call(
        functools.partial(heat_kernel, n_g, n_o, cap, span),
        out_shape=pltpu.VMEM((STRIP, quarter), jnp.float32),
        in_specs=[hbm] * 5,
        out_specs=vmem,
        scratch_shapes=[
            pltpu.VMEM(tile_row.shape, jnp.int32),
            pltpu.VMEM(pixel_col.shape, jnp.int32),
            pltpu.VMEM(weight.shape, weight.dtype),
            pltpu.SMEM(counts.shape, jnp.int32),
            pltpu.SMEM(kernel.shape, jnp.float32),
            pltpu.VMEM((2, slots), jnp.float32),
            pltpu.VMEM((n, 2, span), jnp.float32),
            pltpu.VMEM((tiles * STRIP, LANES), jnp.float32),
            pltpu.VMEM((2, REACH, width), jnp.bfloat16),
            pltpu.VMEM((2, REACH, width), jnp.bfloat16),
            pltpu.VMEM((TAPS, STRIP, width), jnp.float32),
            pltpu.VMEM((REACH, STRIP, width), jnp.float32),
            pltpu.VMEM((REACH * TAPS, STRIP, 128), jnp.float32),
            pltpu.SemaphoreType.DMA((5,)),
            pltpu.SemaphoreType.DMA((n,)),
            pltpu.SemaphoreType.DMA((n,)),
            pltpu.SemaphoreType.DMA((2,)),
            pltpu.SemaphoreType.DMA((2,)),
        ],
        compiler_params=pltpu.CompilerParams(collective_id=0, has_side_effects=True),
    )(tile_row, pixel_col, weight, counts, kernel)


def solution(mesh):
    placed = (
        P("grp", "own", None),
        P("grp", "own", None),
        P("grp", "own", None),
        P("grp", "own", None),
        P(),
    )
    return jax.shard_map(
        per_device, mesh=mesh, in_specs=placed, out_specs=P("own", "grp"), check_vma=False
    )
```
